256 devices in a mesh: row: 16 (over z_hi, y, core), col: 16 (over x, z_lo).
Axes of the slice: x: 4, y: 4, z: 8 (z_hi: 2, z_lo: 4; z = z_hi * 4 + z_lo), core: 2. Of those that a mesh axis runs over, the one named last changes fastest.
Arguments:
- series: float32 [16384, 2048], P(('row', 'col'))
- lengths: int32 [16384], P(('row', 'col')), may hold values from 512 to 2048
- starts: int32 [16384], P(('row', 'col')), may hold values from 0 to 1536, as said below
Outputs:
- correlation: float32 [16384, 16384], P('row', 'col')
The draws below stay inside these ranges and needn't reach their ends.
Inputs may be any that keep to these rules, and one draw needn't show every extreme that they name: starts[s] + lengths[s] <= 2048 for every series.
All inputs are finite; a program needn't handle non-finite values.
Results may differ from the reference program's by a relative error of at most 0.0012.
Values may be sent and summed in bfloat16 or wider, within the bound.
A program may use at most 64 MiB of HBM per device.

```python
import math
import jax
import jax.numpy as jnp
from jax import lax

STEPS = 2048
SERIES = 16384
N_ROW = 16


factor_total = 24


def draw_series(key, part):
    subkeys = jax.random.split(jax.random.fold_in(key, 11), 6)
    factors = jax.random.normal(subkeys[0], (factor_total, STEPS), jnp.float32)
    loadings = jax.random.normal(subkeys[1], (SERIES, factor_total), jnp.float32)
    common = jnp.dot(loadings, factors) / math.sqrt(factor_total)
    column_scale = jnp.exp(jax.random.uniform(subkeys[2], (1, STEPS), jnp.float32, 0.0, math.log(3.0)))
    noise = jax.random.normal(subkeys[3], (SERIES, STEPS), jnp.float32)
    level = jax.random.uniform(subkeys[4], (SERIES, 1), jnp.float32, -3.0, 3.0)
    row_scale = jnp.exp(jax.random.uniform(subkeys[5], (SERIES, 1), jnp.float32, 0.0, math.log(10.0)))
    values = level + row_scale * column_scale * (common + 0.7 * noise)
    return values.astype(jnp.float32)


def windows(key):
    subkeys = jax.random.split(jax.random.fold_in(key, 7), 4)
    lengths = jax.random.randint(subkeys[0], (SERIES,), STEPS // 4, STEPS + 1, jnp.int32)
    longest = jax.random.randint(subkeys[1], (), 0, SERIES // 2, jnp.int32)
    shortest = SERIES // 2 + jax.random.randint(subkeys[2], (), 0, SERIES // 2, jnp.int32)
    lengths = lengths.at[longest].set(STEPS).at[shortest].set(STEPS // 4)
    raw_bits = jax.random.randint(subkeys[3], (SERIES,), 0, 1 << 30, jnp.int32)
    starts = raw_bits % (STEPS - lengths + 1)
    starts = starts.at[shortest].set(STEPS - STEPS // 4)
    return (lengths, starts)


def draw_lengths(key, part):
    return windows(key)[0]


def draw_starts(key, part):
    return windows(key)[1]


def setup_inputs(seed: int = 0) -> dict:
    key_of = jax.random.split(jax.random.key(seed), 4)
    return {
        "series": draw_series(jax.random.fold_in(key_of[3], 71), 0),
        "lengths": draw_lengths(jax.random.fold_in(key_of[3], 71), 0),
        "starts": draw_starts(jax.random.fold_in(key_of[3], 71), 0),
    }


def normalize(series, lengths, starts):
    positions = jnp.arange(series.shape[1], dtype=jnp.int32)[None, :]
    inside = ((positions >= starts[:, None]) & (positions < (starts + lengths)[:, None])).astype(jnp.float32)
    valid_count = lengths.astype(jnp.float32)[:, None]
    average = lax.optimization_barrier(jnp.sum(inside * series, axis=1, keepdims=True)) / valid_count
    centered = inside * (series - average)
    variance = lax.optimization_barrier(jnp.sum(centered * centered, axis=1, keepdims=True)) / valid_count
    return (centered / jnp.sqrt(valid_count * (variance + 1e-06))).astype(jnp.bfloat16)

def reference(series, lengths, starts):
    normed = normalize(series, lengths, starts)
    block_rows = SERIES // N_ROW
    blocks = normed.reshape(N_ROW, block_rows, STEPS)

    def one_block(rows_block):
        return lax.dot_general(rows_block, normed, (((1,), (1,)), ((), ())), preferred_element_type=jnp.float32)
    return lax.map(one_block, blocks).reshape(SERIES, SERIES)
```

```python
import functools

import jax
import jax.numpy as jnp
from jax import lax
from jax.experimental import pallas as pl
from jax.experimental.pallas import tpu as pltpu
from jax.sharding import PartitionSpec as P

LANES = 128
SIDE = 4
ALONG_Z = 7
LIMIT = 32
MESH = pl.DeviceIdType.MESH
ORDER = (
    0, 1, 11, 54, 112, 155, 12, 113, 55, 156, 13, 114, 137, 29, 181, 66, 56, 157, 138, 30,
    14, 40, 127, 81, 167, 57, 15, 182, 148, 47, 16, 196, 8, 53, 206, 204, 9, 31, 67, 115,
    158, 41, 116, 208, 10, 109, 154, 209, 32, 110, 95, 117, 17, 27, 224, 58, 18, 5, 68,
    139, 52, 183, 225, 207, 82, 205, 140, 28, 6, 111, 39, 168, 19, 212, 197, 118, 216, 159,
    96, 7, 48, 135, 64, 119, 69, 106, 153, 136, 107, 179, 184, 210, 128, 228, 83, 79, 232,
    213, 120, 217, 65, 165, 70, 180, 169, 2, 185, 80, 20, 84, 21, 51, 22, 194, 108, 3, 166,
    59, 33, 34, 170, 4, 195, 198, 199, 211, 93, 94, 149, 25, 26, 46, 97, 98, 233, 220, 229,
    226, 42, 38, 121, 122, 123, 126, 160, 218, 103, 104, 105, 152, 214, 71, 72, 62, 63,
    141, 142, 177, 178, 186, 187, 227, 147, 85, 77, 78, 133, 134, 86, 221, 236, 163, 164,
    171, 172, 125, 129, 43, 219, 23, 24, 37, 200, 201, 192, 193, 91, 92, 99, 100, 234, 35,
    36, 49, 215, 230, 45, 237, 60, 61, 175, 176, 222, 143, 144, 75, 76, 131, 146, 235, 130,
    124, 73, 74, 132, 231, 188, 189, 161, 162, 150, 190, 191, 87, 88, 89, 90, 223, 173,
    174, 202, 203, 44, 50, 238, 101, 102, 145, 239, 151,
)


def column_of(row_values):
    n = row_values.shape[1]
    here = lax.broadcasted_iota(jnp.int32, (n, n), 0)
    there = lax.broadcasted_iota(jnp.int32, (n, n), 1)
    picked = jnp.where(here == there, jnp.broadcast_to(row_values, (n, n)), 0)
    return jnp.sum(picked, axis=1, keepdims=True)


def normalize(series, lengths, starts):
    positions = lax.broadcasted_iota(jnp.int32, series.shape, 1)
    inside = (positions >= starts) & (positions < starts + lengths)
    valid_count = lengths.astype(jnp.float32)
    average = jnp.sum(jnp.where(inside, series, 0.0), axis=1, keepdims=True) / valid_count
    centered = jnp.where(inside, series - average, 0.0)
    variance = jnp.sum(centered * centered, axis=1, keepdims=True) / valid_count
    return (centered / jnp.sqrt(valid_count * (variance + 1e-06))).astype(jnp.bfloat16)


def pick(condition, a, b):
    if isinstance(condition, (bool, int)):
        return a if condition else b
    return jnp.where(condition, a, b)


def columns_of(steps):
    half, along = steps // 2, ALONG_Z * LANES
    return [
        (0, along), (along, half), (half, half + along), (half + along, steps),
        (0, half), (half, steps),
    ]


def events_of(r, c):
    n = SIDE
    zh, y, k = r // (2 * n), r // 2 % n, r % 2
    x, z = c // n, c % n

    def row_at(zh, y, k):
        return zh * (2 * n) + y % n * 2 + k

    def col_at(x, z):
        return x % n * n + z

    def c_y(row):
        return row // 2 % n

    events = []
    go = {
        "x+": (True, r, col_at(x + 1, z)),
        "x-": (True, r, col_at(x + n - 1, z)),
        "z+": (z < n - 1, r, c + 1),
        "z-": (z > 0, r, c - 1),
    }

    home_x, home_z = r // n, r % n
    d = (home_x - x + n) % n
    core = d % 2
    target = pick(d == 0, n * n + c, 2 * n * n + d // 3)
    here = (z == home_z) & (z == 0) & (core == k)
    for half in (4, 5):
        sends = [
            (True, c, target, half, row_at((zh + 1) % 2, y + z, core), col_at(x, home_z)),
            (1 - pick(here, 1, 0) == 1, c, target, half, row_at(zh, y + z, core),
             col_at(x, home_z)),
            (here, c, target, half, None, None),
            (here & (d != 0), c, n * n + c, half, r, col_at(home_x, z)),
        ]
        for row in (row_at(zh, y + 1, k), row_at(zh, y + n - 1, k), row_at(zh, y, 1 - k)):
            sends.append((here & (d == 0), n * n + c, n * n + c, half, row, c))
        events.append((("own", half), True, None, sends, []))

    for piece in range(4):
        first, second = piece % 2 == 0, piece // 2
        for dx in (0, 3, 1, 2):
            for dz in range(1 - n, n):
                slot = col_at(x + dx, 0) + z + dz
                valid = (z + dz >= 0) & (z + dz < n)
                def ways(*names):
                    return [
                        (go[way][0], slot, slot, piece, go[way][1], go[way][2])
                        for way in names
                    ]

                def add(kind, sends):
                    events.append(
                        ((kind, dx, dz, piece), valid, None, sends, [(slot, piece)])
                    )

                z_ways = (["z+"] if dz <= 0 else []) + (["z-"] if dz >= 0 else [])
                wait = None if dx == 0 and dz == 0 else (slot, piece)
                urgent = ways(*z_ways) if dx == 0 else []
                events.append((("left", dx, dz, piece), valid, wait, urgent, []))
                if first or dz == 0:
                    if dx == 0:
                        add("near", ways("x+" if second == 0 else "x-"))
                        add("side", ways("x-" if second == 0 else "x+"))
                    elif dx == 3 and second == 0:
                        add("far", ways("x+"))
                    elif dx == 1 and second == 1:
                        add("far", ways("x-"))
                if not first and dx != 0:
                    add("over", ways(*z_ways))

    for j in range(2):
        for half in (4, 5):
            d = 2 - k + 2 * j
            slot = 2 * n * n + j
            from_z = (y - c_y((x + d) % n * n + z) + n) % n
            sends = [(True, slot, n * n + x * n + from_z, half, r, col_at(x + d, z))]
            panel = (x + d) % n * n + z
            arrives = (r != panel) | (z != 0)
            valid = arrives if j == 0 else arrives & (k == 1)
            events.append((("pass", j, half), valid, (slot, half), sends, []))

    for j in range(2):
        for dy in (0, 3, 1, 2):
            for half in (4, 5):
                from_z = (y + dy - c_y(c) + n) % n
                slot = n * n + (x + k + 2 * j) % n * n + from_z
                up = (True, slot, slot, half, row_at(zh, y + 1, k), c)
                down = (True, slot, slot, half, row_at(zh, y + n - 1, k), c)
                across = (True, slot, slot, half, row_at(zh, y, 1 - k), c)
                sends = []
                if dy == 0:
                    sends = [up, down] if half == 4 else [down, up]
                elif dy == 3 and half == 4:
                    sends = [up]
                elif dy == 1 and half == 5:
                    sends = [down]
                valid = True
                if dy == 0 and j == 0:
                    valid = (k == 1) | (r != c) | (z != 0)
                events.append(
                    (("right", j, dy, half), valid, (slot, half), sends + [across], [])
                )
                slot = n * n + (x + 1 - k + 2 * j) % n * n + from_z
                events.append((("across", j, dy, half), True, (slot, half), [], []))
    if ORDER:
        events = [events[i] for i in ORDER]
    return events


def peers_of(r, c):
    n = SIDE
    zh, y, k = r // (2 * n), r // 2 % n, r % 2
    x, z = c // n, c % n
    around = [(True, r, (c + n) % (n * n)), (True, r, (c + 3 * n) % (n * n))]
    around += [(z < n - 1, r, c + 1), (z > 0, r, c - 1)]
    for dy in (1, n - 1):
        around.append((True, zh * 2 * n + (y + dy) % n * 2 + k, c))
    around.append((True, r + 1 - 2 * k, c))
    around.append((k == 0, r, (c + 2 * n) % (n * n)))
    home_x, home_z = r // n, r % n
    core = (home_x - x + n) % n % 2
    into, out = list(around), list(around)
    for group in range(2):
        row, col = group * 2 * n + (y + z) % n * 2 + core, x * n + home_z
        out.append(((row != r) | (col != c), row, col))
        row = (x + k + 2 * group) % n * n + z
        col = x * n + (y - row // 2 % n + n) % n
        into.append(((row != r) | (col != c), row, col))
    return into, out


def kernel(columns, series_ref, windows_ref, slab, recv, send):
    r = lax.axis_index("row")
    c = lax.axis_index("col")
    n = SIDE

    into, out = peers_of(r, c)
    barrier = pltpu.get_barrier_semaphore()
    for condition, row, col in into:

        @pl.when(condition)
        def _(row=row, col=col):
            pl.semaphore_signal(
                barrier, inc=1, device_id={"row": row, "col": col}, device_id_type=MESH
            )

    slab[c] = normalize(
        series_ref[...], column_of(windows_ref[0:1]), column_of(windows_ref[1:2])
    )
    expected = sum(jnp.where(condition, 1, 0) for condition, _, _ in out)
    pl.semaphore_wait(barrier, expected)

    started = []

    def part(slot, piece):
        lo, hi = columns[piece]
        return slab.at[slot, :, pl.ds(lo, hi - lo)]

    def copy_of(index, source, target, piece, row, col):
        return pltpu.make_async_remote_copy(
            src_ref=part(source, piece),
            dst_ref=part(target, piece),
            send_sem=send.at[index],
            recv_sem=recv.at[target, piece],
            device_id={"row": row, "col": col},
            device_id_type=MESH,
        )

    def guarded(condition, do):
        if condition is True:
            do()
        else:
            pl.when(condition)(do)

    def handle(wait, sends):
        if wait is not None:

            def receive():
                copy_of(0, wait[0], wait[0], wait[1], r, c).wait_recv()

            receive()
        for condition, source, target, piece, row, col in sends:
            if row is None:

                def keep(source=source, target=target, piece=piece):
                    part(target, piece)[...] = part(source, piece)[...]

                guarded(condition, keep)
                continue
            index = len(started)
            copy = functools.partial(copy_of, index, source, target, piece, row, col)
            guarded(condition, lambda copy=copy: copy().start())
            started.append((condition, copy))

    for name, condition, wait, sends, _ in events_of(r, c):
        before = len(started)
        guarded(condition, lambda: handle(wait, sends))
        if condition is not True:
            started[before:] = [
                (condition if own is True else condition & own, copy)
                for own, copy in started[before:]
            ]

    for condition, copy in started:
        guarded(condition, lambda copy=copy: copy().wait_send())


def count_sends():
    return sum(len(event[3]) for event in events_of(0, 0))


def multiply(slab, out_ref):
    half, rows_dev, steps = SIDE * SIDE, slab.shape[1], slab.shape[2]
    left = slab[:half].reshape(half * rows_dev, steps)
    group = max(1, 256 // rows_dev)
    for g in range(half // group):
        right = slab[half + g * group : half + (g + 1) * group]
        out_ref[:, g * group * rows_dev : (g + 1) * group * rows_dev] = lax.dot_general(
            left, right.reshape(group * rows_dev, steps), (((1,), (1,)), ((), ())),
            preferred_element_type=jnp.float32,
        )


def on_device(series, lengths, starts):
    rows_dev, steps = series.shape
    blocks = SIDE * SIDE
    vmem = pl.BlockSpec(memory_space=pltpu.VMEM)
    columns = columns_of(steps)
    slots = 2 * blocks + 2
    slab = pl.pallas_call(
        functools.partial(kernel, columns),
        out_shape=jax.ShapeDtypeStruct((slots, rows_dev, steps), jnp.bfloat16),
        in_specs=[vmem] * 2,
        out_specs=vmem,
        scratch_shapes=[
            pltpu.SemaphoreType.DMA((slots, len(columns))),
            pltpu.SemaphoreType.DMA((count_sends(),)),
        ],
        compiler_params=pltpu.CompilerParams(
            collective_id=0, has_side_effects=True, vmem_limit_bytes=LIMIT * 2**20
        ),
    )(series, jnp.stack([lengths, starts]))
    rows = blocks * rows_dev
    return pl.pallas_call(
        multiply,
        grid=(1,),
        out_shape=jax.ShapeDtypeStruct((rows, rows), jnp.float32),
        in_specs=[vmem],
        out_specs=pl.BlockSpec((rows, rows), lambda i: (i, 0)),
        compiler_params=pltpu.CompilerParams(vmem_limit_bytes=LIMIT * 2**20),
    )(slab)


def solution(mesh):
    in_specs = (P(("row", "col"), None), P(("row", "col")), P(("row", "col")))
    out_specs = P("row", "col")
    return jax.shard_map(
        on_device, mesh=mesh, in_specs=in_specs, out_specs=out_specs, check_vma=False,
    )
```

```python
import functools

import jax
import jax.numpy as jnp
from jax import lax
from jax.experimental import pallas as pl
from jax.experimental.pallas import tpu as pltpu
from jax.sharding import PartitionSpec as P

LANES = 128
SIDE = 4
ALONG_Z = 7
LIMIT = 32
OUT_PARTS = 4
MESH = pl.DeviceIdType.MESH
ORDER = (
    0, 5, 3, 160, 161, 1, 60, 58, 59, 16, 118, 116, 15, 17, 117, 186, 120, 2, 34, 61, 71,
    72, 19, 201, 119, 86, 113, 172, 20, 208, 18, 14, 12, 68, 114, 99, 200, 115, 144, 36, 4,
    122, 224, 111, 13, 112, 45, 170, 100, 225, 121, 9, 142, 35, 97, 203, 57, 98, 11, 23,
    22, 10, 210, 21, 110, 123, 187, 7, 32, 204, 31, 127, 8, 51, 73, 126, 108, 220, 159,
    226, 109, 84, 56, 26, 153, 6, 216, 80, 184, 174, 83, 140, 199, 25, 62, 63, 147, 202,
    228, 236, 217, 189, 95, 148, 138, 124, 33, 171, 205, 211, 178, 222, 212, 135, 82, 182,
    176, 102, 177, 96, 130, 206, 103, 81, 79, 229, 74, 29, 42, 69, 40, 188, 46, 152, 146,
    167, 94, 232, 28, 213, 197, 41, 139, 30, 175, 38, 137, 101, 87, 143, 162, 214, 237,
    163, 132, 105, 76, 47, 44, 169, 75, 221, 166, 54, 194, 37, 158, 128, 125, 43, 218, 155,
    196, 90, 136, 88, 89, 65, 107, 85, 151, 180, 24, 168, 104, 179, 230, 67, 238, 209, 133,
    92, 191, 234, 185, 70, 91, 183, 198, 227, 223, 157, 215, 66, 231, 55, 207, 77, 106,
    192, 181, 219, 49, 27, 173, 235, 78, 165, 134, 131, 145, 50, 39, 195, 190, 156, 141,
    193, 149, 53, 233, 150, 129, 164, 239, 64, 52, 154, 48, 93,
)


def column_of(row_values):
    n = row_values.shape[1]
    here = lax.broadcasted_iota(jnp.int32, (n, n), 0)
    there = lax.broadcasted_iota(jnp.int32, (n, n), 1)
    picked = jnp.where(here == there, jnp.broadcast_to(row_values, (n, n)), 0)
    return jnp.sum(picked, axis=1, keepdims=True)


def normalize(series, lengths, starts):
    positions = lax.broadcasted_iota(jnp.int32, series.shape, 1)
    inside = (positions >= starts) & (positions < starts + lengths)
    valid_count = lengths.astype(jnp.float32)
    average = jnp.sum(jnp.where(inside, series, 0.0), axis=1, keepdims=True) / valid_count
    centered = jnp.where(inside, series - average, 0.0)
    variance = jnp.sum(centered * centered, axis=1, keepdims=True) / valid_count
    return (centered / jnp.sqrt(valid_count * (variance + 1e-06))).astype(jnp.bfloat16)


def pick(condition, a, b):
    if isinstance(condition, (bool, int)):
        return a if condition else b
    return jnp.where(condition, a, b)


def columns_of(steps):
    half, along = steps // 2, ALONG_Z * LANES
    return [
        (0, along), (along, half), (half, half + along), (half + along, steps),
        (0, half), (half, steps),
    ]


def events_of(r, c):
    n = SIDE
    zh, y, k = r // (2 * n), r // 2 % n, r % 2
    x, z = c // n, c % n

    def row_at(zh, y, k):
        return zh * (2 * n) + y % n * 2 + k

    def col_at(x, z):
        return x % n * n + z

    def c_y(row):
        return row // 2 % n

    events = []
    go = {
        "x+": (True, r, col_at(x + 1, z)),
        "x-": (True, r, col_at(x + n - 1, z)),
        "z+": (z < n - 1, r, c + 1),
        "z-": (z > 0, r, c - 1),
    }

    for half in (4, 5):
        sends = [(z != 0, c, 2 * n * n, half, row_at(zh, y + z, k), c)]
        events.append((("own", half), True, None, sends, []))

    panel = row_at(zh, y + n - z, k)
    home_x, home_z = panel // n, panel % n
    core = (home_x + x) % 2
    here = (home_x == x) & (home_z == z) & (k == 0)
    for half in (4, 5):
        for kind in ("moved", "stays"):
            source = 2 * n * n if kind == "moved" else c
            slot = n * n + c
            sends = [
                (True, source, slot, half, row_at((zh + 1) % 2, y, core),
                 col_at(home_x, home_z)),
                (pick(here, 0, 1) == 1, source, slot, half, row_at(zh, y, core),
                 col_at(home_x, home_z)),
                (here, source, slot, half, None, None),
            ]
            for row in (row_at(zh, y + 2, k), row_at(zh, y + 1, k), row_at(zh, y + n - 1, k),
                        row_at(zh, y, 1 - k)):
                sends.append((here, slot, slot, half, row, c))
            valid, wait = (z != 0, (2 * n * n, half)) if kind == "moved" else (z == 0, None)
            events.append(((kind, half), valid, wait, sends, []))

    for piece in range(4):
        first, second = piece % 2 == 0, piece // 2
        for dx in (0, 3, 1, 2):
            for dz in range(1 - n, n):
                slot = col_at(x + dx, 0) + z + dz
                valid = (z + dz >= 0) & (z + dz < n)
                def ways(*names):
                    return [
                        (go[way][0], slot, slot, piece, go[way][1], go[way][2])
                        for way in names
                    ]

                def add(kind, sends):
                    events.append(
                        ((kind, dx, dz, piece), valid, None, sends, [(slot, piece)])
                    )

                z_ways = (["z+"] if dz <= 0 else []) + (["z-"] if dz >= 0 else [])
                wait = None if dx == 0 and dz == 0 else (slot, piece)
                urgent = ways(*z_ways) if dx == 0 else []
                events.append((("left", dx, dz, piece), valid, wait, urgent, []))
                if first or dz == 0:
                    if dx == 0:
                        add("near", ways("x+" if second == 0 else "x-"))
                        add("side", ways("x-" if second == 0 else "x+"))
                    elif dx == 3 and second == 0:
                        add("far", ways("x+"))
                    elif dx == 1 and second == 1:
                        add("far", ways("x-"))
                if not first and dx != 0:
                    add("over", ways(*z_ways))

    for j in range(2):
        for dy in (0, 3, 1, 2):
            for half in (4, 5):
                from_z = (y + dy - c_y(c) + n) % n
                slot = n * n + (x + k + 2 * j) % n * n + from_z
                up = (True, slot, slot, half, row_at(zh, y + 1, k), c)
                down = (True, slot, slot, half, row_at(zh, y + n - 1, k), c)
                across = (True, slot, slot, half, row_at(zh, y, 1 - k), c)
                sends = []
                if dy == 0:
                    beyond = (True, slot, slot, half, row_at(zh, y + 2, k), c)
                    sends = [beyond, up, down]
                valid = True
                if dy == 0 and j == 0:
                    valid = pick((k == 0) & (panel == c), 0, 1) == 1
                events.append(
                    (("right", j, dy, half), valid, (slot, half), sends + [across], [])
                )
                slot = n * n + (x + 1 - k + 2 * j) % n * n + from_z
                events.append((("across", j, dy, half), True, (slot, half), [], []))
    if ORDER:
        events = [events[i] for i in ORDER]
    waited = set()
    for i, (name, valid, wait, sends, needs) in enumerate(events):
        if name[0] in ("left", "near", "side", "far", "over"):
            own = name[1] == 0 and name[2] == 0
            first = not own and name[1:] not in waited
            waited.add(name[1:])
            arrival = needs[0] if needs else wait
            events[i] = (name, valid, arrival if first else None, sends, needs)
    return events


def peers_of(r, c):
    n = SIDE
    zh, y, k = r // (2 * n), r // 2 % n, r % 2
    x, z = c // n, c % n
    around = [(True, r, (c + n) % (n * n)), (True, r, (c + 3 * n) % (n * n))]
    around += [(z < n - 1, r, c + 1), (z > 0, r, c - 1)]
    for dy in (1, 2, n - 1):
        around.append((True, zh * 2 * n + (y + dy) % n * 2 + k, c))
    around.append((True, r + 1 - 2 * k, c))
    into, out = list(around), list(around)

    def row_at(zh, y, k):
        return zh * (2 * n) + y % n * 2 + k

    out.append((z != 0, row_at(zh, y + z, k), c))
    into.append((z != 0, row_at(zh, y + n - z, k), c))
    panel = row_at(zh, y + n - z, k)
    for group in range(2):
        row, col = row_at(group, y, (panel // n + x) % 2), panel
        out.append(((row != r) | (col != c), row, col))
        from_z = (y + n - c // 2 % n) % n
        row = row_at(c // (2 * n), y, c % 2)
        col = (x + k + 2 * group) % n * n + from_z
        into.append(((row != r) | (col != c), row, col))
    return into, out


def kernel(
    columns, series_hbm, lengths_hbm, starts_hbm, slab,
    series_ref, lengths_ref, starts_ref, recv, send, load,
):
    r = lax.axis_index("row")
    c = lax.axis_index("col")
    n = SIDE

    loads = [
        pltpu.make_async_copy(source, target, load.at[i])
        for i, (source, target) in enumerate((
            (lengths_hbm, lengths_ref), (starts_hbm, starts_ref), (series_hbm, series_ref),
        ))
    ]
    for copy in loads:
        copy.start()
    into, out = peers_of(r, c)
    barrier = pltpu.get_barrier_semaphore()
    for condition, row, col in into:

        @pl.when(condition)
        def _(row=row, col=col):
            pl.semaphore_signal(
                barrier, inc=1, device_id={"row": row, "col": col}, device_id_type=MESH
            )

    for copy in loads:
        copy.wait()
    slab[c] = normalize(
        series_ref[...], column_of(lengths_ref[...]), column_of(starts_ref[...])
    )
    expected = sum(jnp.where(condition, 1, 0) for condition, _, _ in out)
    pl.semaphore_wait(barrier, expected)

    started = []

    def part(slot, piece):
        lo, hi = columns[piece]
        return slab.at[slot, :, pl.ds(lo, hi - lo)]

    def copy_of(index, source, target, piece, row, col):
        return pltpu.make_async_remote_copy(
            src_ref=part(source, piece),
            dst_ref=part(target, piece),
            send_sem=send.at[index],
            recv_sem=recv.at[target, piece],
            device_id={"row": row, "col": col},
            device_id_type=MESH,
        )

    def guarded(condition, do):
        if condition is True:
            do()
        else:
            pl.when(condition)(do)

    def handle(wait, sends):
        if wait is not None:

            def receive():
                copy_of(0, wait[0], wait[0], wait[1], r, c).wait_recv()

            receive()
        for condition, source, target, piece, row, col in sends:
            if row is None:

                def keep(source=source, target=target, piece=piece):
                    part(target, piece)[...] = part(source, piece)[...]

                guarded(condition, keep)
                continue
            index = len(started)
            copy = functools.partial(copy_of, index, source, target, piece, row, col)
            guarded(condition, lambda copy=copy: copy().start())
            started.append((condition, copy))

    for name, condition, wait, sends, _ in events_of(r, c):
        before = len(started)
        guarded(condition, lambda: handle(wait, sends))
        if condition is not True:
            started[before:] = [
                (condition if own is True else condition & own, copy)
                for own, copy in started[before:]
            ]

    for condition, copy in started:
        guarded(condition, lambda copy=copy: copy().wait_send())


def count_sends():
    return sum(len(event[3]) for event in events_of(0, 0))


def multiply(slab, out_ref):
    half, rows_dev, steps = SIDE * SIDE, slab.shape[1], slab.shape[2]
    left = slab[:half].reshape(half * rows_dev, steps)
    group = out_ref.shape[1] // rows_dev
    right = slab[pl.ds(half + pl.program_id(0) * group, group)]
    out_ref[...] = lax.dot_general(
        left, right.reshape(group * rows_dev, steps), (((1,), (1,)), ((), ())),
        preferred_element_type=jnp.float32,
    )


def on_device(series, lengths, starts):
    rows_dev, steps = series.shape
    blocks = SIDE * SIDE
    vmem = pl.BlockSpec(memory_space=pltpu.VMEM)
    columns = columns_of(steps)
    slots = 2 * blocks + 1
    in_hbm = [
        pltpu.with_memory_space_constraint(array, pltpu.HBM)
        for array in (series, lengths.reshape(1, rows_dev), starts.reshape(1, rows_dev))
    ]
    slab = pl.pallas_call(
        functools.partial(kernel, columns),
        out_shape=jax.ShapeDtypeStruct((slots, rows_dev, steps), jnp.bfloat16),
        in_specs=[pl.BlockSpec(memory_space=pltpu.HBM)] * 3,
        out_specs=vmem,
        scratch_shapes=[
            pltpu.VMEM((rows_dev, steps), jnp.float32),
            pltpu.VMEM((1, rows_dev), jnp.int32),
            pltpu.VMEM((1, rows_dev), jnp.int32),
            pltpu.SemaphoreType.DMA((slots, len(columns))),
            pltpu.SemaphoreType.DMA((count_sends(),)),
            pltpu.SemaphoreType.DMA((3,)),
        ],
        compiler_params=pltpu.CompilerParams(
            collective_id=0, has_side_effects=True, vmem_limit_bytes=LIMIT * 2**20
        ),
    )(*in_hbm)
    rows = blocks * rows_dev
    return pl.pallas_call(
        multiply,
        grid=(OUT_PARTS,),
        out_shape=jax.ShapeDtypeStruct((rows, rows), jnp.float32),
        in_specs=[vmem],
        out_specs=pl.BlockSpec((rows, rows // OUT_PARTS), lambda i: (0, i)),
        compiler_params=pltpu.CompilerParams(vmem_limit_bytes=LIMIT * 2**20),
    )(slab)


def solution(mesh):
    in_specs = (P(("row", "col"), None), P(("row", "col")), P(("row", "col")))
    out_specs = P("row", "col")
    return jax.shard_map(
        on_device, mesh=mesh, in_specs=in_specs, out_specs=out_specs, check_vma=False,
    )
```

```python
import functools

import jax
import jax.numpy as jnp
from jax import lax
from jax.experimental import pallas as pl
from jax.experimental.pallas import tpu as pltpu
from jax.sharding import PartitionSpec as P

LANES = 128
SIDE = 4
ALONG_Z = 7
LIMIT = 32
OUT_PARTS = 4
MESH = pl.DeviceIdType.MESH
ORDER = (
    161, 0, 5, 3, 17, 117, 16, 58, 15, 59, 116, 19, 2, 159, 160, 60, 118, 172, 72, 1, 12,
    13, 142, 20, 34, 71, 187, 18, 185, 121, 4, 186, 208, 115, 22, 114, 120, 11, 23, 73, 10,
    14, 224, 86, 8, 7, 44, 9, 113, 36, 119, 210, 122, 123, 57, 173, 220, 189, 85, 32, 110,
    170, 112, 169, 124, 126, 111, 225, 61, 56, 84, 69, 127, 21, 211, 144, 201, 216, 191,
    168, 100, 226, 25, 174, 108, 158, 28, 51, 125, 203, 74, 184, 66, 190, 182, 152, 83,
    138, 148, 102, 98, 221, 183, 193, 227, 42, 199, 81, 146, 212, 26, 131, 67, 171, 38,
    143, 175, 179, 62, 140, 218, 82, 40, 136, 30, 37, 180, 147, 24, 205, 181, 177, 167,
    157, 228, 232, 155, 29, 178, 137, 236, 209, 88, 176, 197, 222, 96, 33, 166, 106, 109,
    104, 207, 99, 198, 196, 188, 134, 162, 202, 75, 68, 35, 39, 214, 238, 230, 95, 48, 101,
    90, 49, 105, 206, 163, 94, 55, 204, 234, 237, 63, 79, 43, 156, 45, 107, 91, 132, 65,
    153, 97, 80, 233, 135, 192, 64, 195, 223, 76, 231, 77, 6, 78, 129, 27, 215, 200, 31,
    239, 194, 93, 54, 165, 150, 154, 145, 46, 141, 70, 149, 128, 213, 130, 164, 229, 89,
    219, 53, 92, 133, 151, 52, 103, 47, 87, 217, 50, 139, 41, 235,
)


def column_of(row_values):
    n = row_values.shape[1]
    here = lax.broadcasted_iota(jnp.int32, (n, n), 0)
    there = lax.broadcasted_iota(jnp.int32, (n, n), 1)
    picked = jnp.where(here == there, jnp.broadcast_to(row_values, (n, n)), 0)
    return jnp.sum(picked, axis=1, keepdims=True)


def normalize(series, lengths, starts):
    positions = lax.broadcasted_iota(jnp.int32, series.shape, 1)
    inside = (positions >= starts) & (positions < starts + lengths)
    valid_count = lengths.astype(jnp.float32)
    average = jnp.sum(jnp.where(inside, series, 0.0), axis=1, keepdims=True) / valid_count
    centered = jnp.where(inside, series - average, 0.0)
    variance = jnp.sum(centered * centered, axis=1, keepdims=True) / valid_count
    return (centered / jnp.sqrt(valid_count * (variance + 1e-06))).astype(jnp.bfloat16)


def pick(condition, a, b):
    if isinstance(condition, (bool, int)):
        return a if condition else b
    return jnp.where(condition, a, b)


def columns_of(steps):
    half, along = steps // 2, ALONG_Z * LANES
    return [
        (0, along), (along, half), (half, half + along), (half + along, steps),
        (0, half), (half, steps),
    ]


def events_of(r, c):
    n = SIDE
    zh, y, k = r // (2 * n), r // 2 % n, r % 2
    x, z = c // n, c % n

    def row_at(zh, y, k):
        return zh * (2 * n) + y % n * 2 + k

    def col_at(x, z):
        return x % n * n + z

    def c_y(row):
        return row // 2 % n

    events = []
    go = {
        "x+": (True, r, col_at(x + 1, z)),
        "x-": (True, r, col_at(x + n - 1, z)),
        "z+": (z < n - 1, r, c + 1),
        "z-": (z > 0, r, c - 1),
    }

    for half in (4, 5):
        sends = [(z != 0, c, 2 * n * n, half, row_at(zh, y + z, k), c)]
        events.append((("own", half), True, None, sends, []))

    panel = row_at(zh, y + n - z, k)
    home_x, home_z = panel // n, panel % n
    core = (home_x + x) % 2
    here = (home_x == x) & (home_z == z) & (k == 0)
    for half in (4, 5):
        for kind in ("moved", "stays"):
            source = 2 * n * n if kind == "moved" else c
            slot = n * n + c
            sends = [
                (True, source, slot, half, row_at((zh + 1) % 2, y, core),
                 col_at(home_x, home_z)),
                (pick(here, 0, 1) == 1, source, slot, half, row_at(zh, y, core),
                 col_at(home_x, home_z)),
                (here, source, slot, half, None, None),
            ]
            for row in (row_at(zh, y + 2, k), row_at(zh, y + 1, k), row_at(zh, y + n - 1, k),
                        row_at(zh, y, 1 - k)):
                sends.append((here, slot, slot, half, row, c))
            valid, wait = (z != 0, (2 * n * n, half)) if kind == "moved" else (z == 0, None)
            events.append(((kind, half), valid, wait, sends, []))

    for piece in range(4):
        first, second = piece % 2 == 0, piece // 2
        for dx in (0, 3, 1, 2):
            for dz in range(1 - n, n):
                slot = col_at(x + dx, 0) + z + dz
                valid = (z + dz >= 0) & (z + dz < n)
                def ways(*names):
                    return [
                        (go[way][0], slot, slot, piece, go[way][1], go[way][2])
                        for way in names
                    ]

                def add(kind, sends):
                    events.append(
                        ((kind, dx, dz, piece), valid, None, sends, [(slot, piece)])
                    )

                z_ways = (["z+"] if dz <= 0 else []) + (["z-"] if dz >= 0 else [])
                wait = None if dx == 0 and dz == 0 else (slot, piece)
                urgent = ways(*z_ways) if dx == 0 else []
                events.append((("left", dx, dz, piece), valid, wait, urgent, []))
                if first or dz == 0:
                    if dx == 0:
                        add("near", ways("x+" if second == 0 else "x-"))
                        add("side", ways("x-" if second == 0 else "x+"))
                    elif dx == 3 and second == 0:
                        add("far", ways("x+"))
                    elif dx == 1 and second == 1:
                        add("far", ways("x-"))
                if not first and dx != 0:
                    add("over", ways(*z_ways))

    for j in range(2):
        for dy in (0, 3, 1, 2):
            for half in (4, 5):
                from_z = (y + dy - c_y(c) + n) % n
                slot = n * n + (x + k + 2 * j) % n * n + from_z
                up = (True, slot, slot, half, row_at(zh, y + 1, k), c)
                down = (True, slot, slot, half, row_at(zh, y + n - 1, k), c)
                across = (True, slot, slot, half, row_at(zh, y, 1 - k), c)
                sends = []
                if dy == 0:
                    beyond = (True, slot, slot, half, row_at(zh, y + 2, k), c)
                    sends = [beyond, up, down]
                valid = True
                if dy == 0 and j == 0:
                    valid = pick((k == 0) & (panel == c), 0, 1) == 1
                events.append(
                    (("right", j, dy, half), valid, (slot, half), sends + [across], [])
                )
                slot = n * n + (x + 1 - k + 2 * j) % n * n + from_z
                events.append((("across", j, dy, half), True, (slot, half), [], []))
    if ORDER:
        events = [events[i] for i in ORDER]
    waited = set()
    for i, (name, valid, wait, sends, needs) in enumerate(events):
        if name[0] in ("left", "near", "side", "far", "over"):
            own = name[1] == 0 and name[2] == 0
            first = not own and name[1:] not in waited
            waited.add(name[1:])
            arrival = needs[0] if needs else wait
            events[i] = (name, valid, arrival if first else None, sends, needs)
    return events


def peers_of(r, c):
    n = SIDE
    zh, y, k = r // (2 * n), r // 2 % n, r % 2
    x, z = c // n, c % n
    around = [(True, r, (c + n) % (n * n)), (True, r, (c + 3 * n) % (n * n))]
    around += [(z < n - 1, r, c + 1), (z > 0, r, c - 1)]
    for dy in (1, 2, n - 1):
        around.append((True, zh * 2 * n + (y + dy) % n * 2 + k, c))
    around.append((True, r + 1 - 2 * k, c))
    into, out = list(around), list(around)

    def row_at(zh, y, k):
        return zh * (2 * n) + y % n * 2 + k

    out.append((z != 0, row_at(zh, y + z, k), c))
    into.append((z != 0, row_at(zh, y + n - z, k), c))
    panel = row_at(zh, y + n - z, k)
    for group in range(2):
        row, col = row_at(group, y, (panel // n + x) % 2), panel
        out.append(((row != r) | (col != c), row, col))
        from_z = (y + n - c // 2 % n) % n
        row = row_at(c // (2 * n), y, c % 2)
        col = (x + k + 2 * group) % n * n + from_z
        into.append(((row != r) | (col != c), row, col))
    return into, out


def kernel(
    columns, steps, series_hbm, lengths_hbm, starts_hbm, slab,
    series_ref, lengths_ref, starts_ref, recv, send, load,
):
    r = lax.axis_index("row")
    c = lax.axis_index("col")
    n = SIDE

    loads = [
        pltpu.make_async_copy(source, target, load.at[i])
        for i, (source, target) in enumerate((
            (lengths_hbm, lengths_ref), (starts_hbm, starts_ref), (series_hbm, series_ref),
        ))
    ]
    for copy in loads:
        copy.start()
    into, out = peers_of(r, c)
    barrier = pltpu.get_barrier_semaphore()
    for condition, row, col in into:

        @pl.when(condition)
        def _(row=row, col=col):
            pl.semaphore_signal(
                barrier, inc=1, device_id={"row": row, "col": col}, device_id_type=MESH
            )

    for copy in loads:
        copy.wait()
    slab[c] = normalize(
        series_ref[...], column_of(lengths_ref[...]), column_of(starts_ref[...])
    )
    expected = sum(jnp.where(condition, 1, 0) for condition, _, _ in out)
    pl.semaphore_wait(barrier, expected)

    def arrival_of(slot, piece):
        if piece < 4:
            return slot * 4 + piece
        return n * n * 4 + (slot - n * n) * 2 + piece - 4

    def part(slot, piece):
        lo, hi = columns[piece]
        return slab.at[slot, :, pl.ds(lo, hi - lo)]

    def copy_of(index, source, target, piece, row, col):
        return pltpu.make_async_remote_copy(
            src_ref=part(source, piece),
            dst_ref=part(target, piece),
            send_sem=send.at[index],
            recv_sem=recv.at[arrival_of(target, piece)],
            device_id={"row": row, "col": col},
            device_id_type=MESH,
        )

    def guarded(condition, do):
        if condition is True:
            do()
        else:
            pl.when(condition)(do)

    def handle(group, wait, sends):
        if wait is not None:

            def receive():
                copy_of(group, wait[0], wait[0], wait[1], r, c).wait_recv()

            receive()
        for condition, source, target, piece, row, col in sends:
            if row is None:

                def keep(source=source, target=target, piece=piece):
                    part(target, piece)[...] = part(source, piece)[...]

                guarded(condition, keep)
                continue
            copy = functools.partial(copy_of, group, source, target, piece, row, col)
            guarded(condition, lambda copy=copy: copy().start())

    groups = {"near": 0, "side": 0, "far": 0, "left": 1, "over": 1}
    for name, condition, wait, sends, _ in events_of(r, c):
        group = groups.get(name[0], 2)
        guarded(condition, functools.partial(handle, group, wait, sends))

    def sent(group, blocks, tiles):
        here = slab.at[pl.ds(0, blocks), :, pl.ds(0, tiles * LANES)]
        pltpu.make_async_remote_copy(
            src_ref=here, dst_ref=here, send_sem=send.at[group], recv_sem=recv.at[0],
            device_id={"row": r, "col": c}, device_id_type=MESH,
        ).wait_send()

    x_tiles, z_tiles = sent_left()
    sent(0, *x_tiles)
    z = c % n
    middle = (z > 0) & (z < n - 1)
    guarded(middle, lambda: sent(1, *z_tiles[1]))
    guarded(jnp.logical_not(middle), lambda: sent(1, *z_tiles[0]))
    rights = 15 + jnp.where(z == 0, 0, 1) + jnp.where(stays_here(r, c), 0, 1)
    for blocks in (15, 16, 17):
        guarded(rights == blocks, lambda blocks=blocks: sent(2, blocks, steps // LANES))


def stays_here(r, c):
    n = SIDE
    y, k = r // 2 % n, r % 2
    return (r // (2 * n) * 2 * n + (y + n - c % n) % n * 2 + k == c) & (k == 0)


def sent_left():
    near = 2 * ALONG_Z
    along_x = SIDE * (2 * near + near) + 3 * (16 - near)
    ends = 16 + 3 * (16 - near)
    return rectangle(along_x), (rectangle(ends), rectangle(5 * ends))


def rectangle(tiles):
    return next(
        (tiles // width, width) for width in range(16, 0, -1)
        if tiles % width == 0 and tiles // width <= 2 * SIDE * SIDE
    )


def multiply(slab, out_ref):
    half, rows_dev, steps = SIDE * SIDE, slab.shape[1], slab.shape[2]
    left = slab[:half].reshape(half * rows_dev, steps)
    group = out_ref.shape[1] // rows_dev
    right = slab[pl.ds(half + pl.program_id(0) * group, group)]
    out_ref[...] = lax.dot_general(
        left, right.reshape(group * rows_dev, steps), (((1,), (1,)), ((), ())),
        preferred_element_type=jnp.float32,
    )


def on_device(series, lengths, starts):
    rows_dev, steps = series.shape
    blocks = SIDE * SIDE
    vmem = pl.BlockSpec(memory_space=pltpu.VMEM)
    columns = columns_of(steps)
    slots = 2 * blocks + 1
    in_hbm = [
        pltpu.with_memory_space_constraint(array, pltpu.HBM)
        for array in (series, lengths.reshape(1, rows_dev), starts.reshape(1, rows_dev))
    ]
    slab = pl.pallas_call(
        functools.partial(kernel, columns, steps),
        out_shape=jax.ShapeDtypeStruct((slots, rows_dev, steps), jnp.bfloat16),
        in_specs=[pl.BlockSpec(memory_space=pltpu.HBM)] * 3,
        out_specs=vmem,
        scratch_shapes=[
            pltpu.VMEM((rows_dev, steps), jnp.float32),
            pltpu.VMEM((1, rows_dev), jnp.int32),
            pltpu.VMEM((1, rows_dev), jnp.int32),
            pltpu.SemaphoreType.DMA((blocks * 4 + (blocks + 1) * 2,)),
            pltpu.SemaphoreType.DMA((3,)),
            pltpu.SemaphoreType.DMA((3,)),
        ],
        compiler_params=pltpu.CompilerParams(
            collective_id=0, has_side_effects=True, vmem_limit_bytes=LIMIT * 2**20
        ),
    )(*in_hbm)
    rows = blocks * rows_dev
    return pl.pallas_call(
        multiply,
        grid=(OUT_PARTS,),
        out_shape=jax.ShapeDtypeStruct((rows, rows), jnp.float32),
        in_specs=[vmem],
        out_specs=pl.BlockSpec((rows, rows // OUT_PARTS), lambda i: (0, i)),
        compiler_params=pltpu.CompilerParams(vmem_limit_bytes=LIMIT * 2**20),
    )(slab)


def solution(mesh):
    in_specs = (P(("row", "col"), None), P(("row", "col")), P(("row", "col")))
    out_specs = P("row", "col")
    return jax.shard_map(
        on_device, mesh=mesh, in_specs=in_specs, out_specs=out_specs, check_vma=False,
    )
```

```python
import functools

import jax
import jax.numpy as jnp
from jax import lax
from jax.experimental import pallas as pl
from jax.experimental.pallas import tpu as pltpu
from jax.sharding import PartitionSpec as P

LANES = 128
SIDE = 4
ALONG_Z = 7
LIMIT = 32
AHEAD = (0, 3, 1)
MESH = pl.DeviceIdType.MESH
ORDER = (
    161, 0, 5, 3, 17, 117, 16, 58, 15, 59, 116, 19, 2, 159, 160, 60, 118, 172, 72, 1, 12,
    13, 142, 20, 34, 71, 187, 18, 185, 121, 4, 186, 208, 115, 22, 114, 120, 11, 23, 73, 10,
    14, 224, 86, 8, 7, 44, 9, 113, 36, 119, 210, 122, 123, 57, 173, 220, 189, 85, 32, 110,
    170, 112, 169, 124, 126, 111, 225, 61, 56, 84, 69, 127, 21, 211, 144, 201, 216, 191,
    168, 100, 226, 25, 174, 108, 158, 28, 51, 125, 203, 74, 184, 66, 190, 182, 152, 83,
    138, 148, 102, 98, 221, 183, 193, 227, 42, 199, 81, 146, 212, 26, 131, 67, 171, 38,
    143, 175, 179, 62, 140, 218, 82, 40, 136, 30, 37, 180, 147, 24, 205, 181, 177, 167,
    157, 228, 232, 155, 29, 178, 137, 236, 209, 88, 176, 197, 222, 96, 33, 166, 106, 109,
    104, 207, 99, 198, 196, 188, 134, 162, 202, 75, 68, 35, 39, 214, 238, 230, 95, 48, 101,
    90, 49, 105, 206, 163, 94, 55, 204, 234, 237, 63, 79, 43, 156, 45, 107, 91, 132, 65,
    153, 97, 80, 233, 135, 192, 64, 195, 223, 76, 231, 77, 6, 78, 129, 27, 215, 200, 31,
    239, 194, 93, 54, 165, 150, 154, 145, 46, 141, 70, 149, 128, 213, 130, 164, 229, 89,
    219, 53, 92, 133, 151, 52, 103, 47, 87, 217, 50, 139, 41, 235,
)


def column_of(row_values):
    n = row_values.shape[1]
    here = lax.broadcasted_iota(jnp.int32, (n, n), 0)
    there = lax.broadcasted_iota(jnp.int32, (n, n), 1)
    picked = jnp.where(here == there, jnp.broadcast_to(row_values, (n, n)), 0)
    return jnp.sum(picked, axis=1, keepdims=True)


def normalize(series, lengths, starts):
    positions = lax.broadcasted_iota(jnp.int32, series.shape, 1)
    inside = (positions >= starts) & (positions < starts + lengths)
    valid_count = lengths.astype(jnp.float32)
    average = jnp.sum(jnp.where(inside, series, 0.0), axis=1, keepdims=True) / valid_count
    centered = jnp.where(inside, series - average, 0.0)
    variance = jnp.sum(centered * centered, axis=1, keepdims=True) / valid_count
    return (centered / jnp.sqrt(valid_count * (variance + 1e-06))).astype(jnp.bfloat16)


def pick(condition, a, b):
    if isinstance(condition, (bool, int)):
        return a if condition else b
    return jnp.where(condition, a, b)


def columns_of(steps):
    half, along = steps // 2, ALONG_Z * LANES
    return [
        (0, along), (along, half), (half, half + along), (half + along, steps),
        (0, half), (half, steps),
    ]


def events_of(r, c):
    n = SIDE
    zh, y, k = r // (2 * n), r // 2 % n, r % 2
    x, z = c // n, c % n

    def row_at(zh, y, k):
        return zh * (2 * n) + y % n * 2 + k

    def col_at(x, z):
        return x % n * n + z

    def c_y(row):
        return row // 2 % n

    events = []
    go = {
        "x+": (True, r, col_at(x + 1, z)),
        "x-": (True, r, col_at(x + n - 1, z)),
        "z+": (z < n - 1, r, c + 1),
        "z-": (z > 0, r, c - 1),
    }

    for half in (4, 5):
        sends = [(z != 0, c, 2 * n * n, half, row_at(zh, y + z, k), c)]
        events.append((("own", half), True, None, sends, []))

    panel = row_at(zh, y + n - z, k)
    home_x, home_z = panel // n, panel % n
    core = (home_x + x) % 2
    here = (home_x == x) & (home_z == z) & (k == 0)
    for half in (4, 5):
        for kind in ("moved", "stays"):
            source = 2 * n * n if kind == "moved" else c
            slot = n * n + c
            sends = [
                (True, source, slot, half, row_at((zh + 1) % 2, y, core),
                 col_at(home_x, home_z)),
                (pick(here, 0, 1) == 1, source, slot, half, row_at(zh, y, core),
                 col_at(home_x, home_z)),
                (here, source, slot, half, None, None),
            ]
            for row in (row_at(zh, y + 2, k), row_at(zh, y + 1, k), row_at(zh, y + n - 1, k),
                        row_at(zh, y, 1 - k)):
                sends.append((here, slot, slot, half, row, c))
            valid, wait = (z != 0, (2 * n * n, half)) if kind == "moved" else (z == 0, None)
            events.append(((kind, half), valid, wait, sends, []))

    for piece in range(4):
        first, second = piece % 2 == 0, piece // 2
        for dx in (0, 3, 1, 2):
            for dz in range(1 - n, n):
                slot = col_at(x + dx, 0) + z + dz
                valid = (z + dz >= 0) & (z + dz < n)
                def ways(*names):
                    return [
                        (go[way][0], slot, slot, piece, go[way][1], go[way][2])
                        for way in names
                    ]

                def add(kind, sends):
                    events.append(
                        ((kind, dx, dz, piece), valid, None, sends, [(slot, piece)])
                    )

                z_ways = (["z+"] if dz <= 0 else []) + (["z-"] if dz >= 0 else [])
                wait = None if dx == 0 and dz == 0 else (slot, piece)
                urgent = ways(*z_ways) if dx == 0 else []
                events.append((("left", dx, dz, piece), valid, wait, urgent, []))
                if first or dz == 0:
                    if dx == 0:
                        add("near", ways("x+" if second == 0 else "x-"))
                        add("side", ways("x-" if second == 0 else "x+"))
                    elif dx == 3 and second == 0:
                        add("far", ways("x+"))
                    elif dx == 1 and second == 1:
                        add("far", ways("x-"))
                if not first and dx != 0:
                    add("over", ways(*z_ways))

    for j in range(2):
        for dy in (0, 3, 1, 2):
            for half in (4, 5):
                from_z = (y + dy - c_y(c) + n) % n
                slot = n * n + (x + k + 2 * j) % n * n + from_z
                up = (True, slot, slot, half, row_at(zh, y + 1, k), c)
                down = (True, slot, slot, half, row_at(zh, y + n - 1, k), c)
                across = (True, slot, slot, half, row_at(zh, y, 1 - k), c)
                sends = []
                if dy == 0:
                    beyond = (True, slot, slot, half, row_at(zh, y + 2, k), c)
                    sends = [beyond, up, down]
                valid = True
                if dy == 0 and j == 0:
                    valid = pick((k == 0) & (panel == c), 0, 1) == 1
                events.append(
                    (("right", j, dy, half), valid, (slot, half), sends + [across], [])
                )
                slot = n * n + (x + 1 - k + 2 * j) % n * n + from_z
                events.append((("across", j, dy, half), True, (slot, half), [], []))
    if ORDER:
        events = [events[i] for i in ORDER]
    events = [e for e in events if e[3]] + [e for e in events if not e[3]]
    waited = set()
    for i, (name, valid, wait, sends, needs) in enumerate(events):
        if name[0] in ("left", "near", "side", "far", "over"):
            own = name[1] == 0 and name[2] == 0
            first = not own and name[1:] not in waited
            waited.add(name[1:])
            arrival = needs[0] if needs else wait
            events[i] = (name, valid, arrival if first else None, sends, needs)
    return events


def peers_of(r, c):
    n = SIDE
    zh, y, k = r // (2 * n), r // 2 % n, r % 2
    x, z = c // n, c % n
    around = [(True, r, (c + n) % (n * n)), (True, r, (c + 3 * n) % (n * n))]
    around += [(z < n - 1, r, c + 1), (z > 0, r, c - 1)]
    for dy in (1, 2, n - 1):
        around.append((True, zh * 2 * n + (y + dy) % n * 2 + k, c))
    around.append((True, r + 1 - 2 * k, c))
    into, out = list(around), list(around)

    def row_at(zh, y, k):
        return zh * (2 * n) + y % n * 2 + k

    out.append((z != 0, row_at(zh, y + z, k), c))
    into.append((z != 0, row_at(zh, y + n - z, k), c))
    panel = row_at(zh, y + n - z, k)
    for group in range(2):
        row, col = row_at(group, y, (panel // n + x) % 2), panel
        out.append(((row != r) | (col != c), row, col))
        from_z = (y + n - c // 2 % n) % n
        row = row_at(c // (2 * n), y, c % 2)
        col = (x + k + 2 * group) % n * n + from_z
        into.append(((row != r) | (col != c), row, col))
    return into, out


def kernel(
    columns, steps, series_hbm, lengths_hbm, starts_hbm, slab, partial,
    series_ref, lengths_ref, starts_ref, recv, send, load,
):
    r = lax.axis_index("row")
    c = lax.axis_index("col")
    n = SIDE

    loads = [
        pltpu.make_async_copy(source, target, load.at[i])
        for i, (source, target) in enumerate((
            (lengths_hbm, lengths_ref), (starts_hbm, starts_ref), (series_hbm, series_ref),
        ))
    ]
    for copy in loads:
        copy.start()
    into, out = peers_of(r, c)
    barrier = pltpu.get_barrier_semaphore()
    for condition, row, col in into:

        @pl.when(condition)
        def _(row=row, col=col):
            pl.semaphore_signal(
                barrier, inc=1, device_id={"row": row, "col": col}, device_id_type=MESH
            )

    for copy in loads:
        copy.wait()
    slab[c] = normalize(
        series_ref[...], column_of(lengths_ref[...]), column_of(starts_ref[...])
    )
    expected = sum(jnp.where(condition, 1, 0) for condition, _, _ in out)
    pl.semaphore_wait(barrier, expected)

    def arrival_of(slot, piece):
        if piece < 4:
            return slot * 4 + piece
        return n * n * 4 + (slot - n * n) * 2 + piece - 4

    def part(slot, piece):
        lo, hi = columns[piece]
        return slab.at[slot, :, pl.ds(lo, hi - lo)]

    def copy_of(index, source, target, piece, row, col):
        return pltpu.make_async_remote_copy(
            src_ref=part(source, piece),
            dst_ref=part(target, piece),
            send_sem=send.at[index],
            recv_sem=recv.at[arrival_of(target, piece)],
            device_id={"row": row, "col": col},
            device_id_type=MESH,
        )

    def guarded(condition, do):
        if condition is True:
            do()
        else:
            pl.when(condition)(do)

    def handle(group, wait, sends):
        if wait is not None:

            def receive():
                copy_of(group, wait[0], wait[0], wait[1], r, c).wait_recv()

            receive()
        for condition, source, target, piece, row, col in sends:
            if row is None:

                def keep(source=source, target=target, piece=piece):
                    part(target, piece)[...] = part(source, piece)[...]

                guarded(condition, keep)
                continue
            copy = functools.partial(copy_of, group, source, target, piece, row, col)
            guarded(condition, lambda copy=copy: copy().start())

    groups = {"near": 0, "side": 0, "far": 0, "left": 1, "over": 1}
    events = events_of(r, c)
    for name, condition, wait, sends, _ in events:
        if sends:
            group = groups.get(name[0], 2)
            guarded(condition, functools.partial(handle, group, wait, sends))

    def arrive(kind, second, dx=None):
        for name, condition, wait, sends, _ in events:
            if sends or name[0] != kind or wait is None:
                continue
            if kind == "across" and name[3] - 4 != second:
                continue
            if kind == "left" and (name[1] != dx or name[3] // 2 != second):
                continue
            guarded(condition, functools.partial(handle, 2, wait, ()))

    arrive("across", 0)
    for dx in AHEAD:
        arrive("left", 0, dx)
        multiply_part(slab, (c // n + dx) % n, 0, steps // 2, None, partial)
    arrive("left", 0, 2)
    for dx in AHEAD + (2,):
        arrive("left", 1, dx)
    arrive("across", 1)

    def sent(group, blocks, tiles):
        here = slab.at[pl.ds(0, blocks), :, pl.ds(0, tiles * LANES)]
        pltpu.make_async_remote_copy(
            src_ref=here, dst_ref=here, send_sem=send.at[group], recv_sem=recv.at[0],
            device_id={"row": r, "col": c}, device_id_type=MESH,
        ).wait_send()

    x_tiles, z_tiles = sent_left()
    sent(0, *x_tiles)
    z = c % n
    middle = (z > 0) & (z < n - 1)
    guarded(middle, lambda: sent(1, *z_tiles[1]))
    guarded(jnp.logical_not(middle), lambda: sent(1, *z_tiles[0]))
    rights = 15 + jnp.where(z == 0, 0, 1) + jnp.where(stays_here(r, c), 0, 1)
    for blocks in (15, 16, 17):
        guarded(rights == blocks, lambda blocks=blocks: sent(2, blocks, steps // LANES))


def stays_here(r, c):
    n = SIDE
    y, k = r // 2 % n, r % 2
    return (r // (2 * n) * 2 * n + (y + n - c % n) % n * 2 + k == c) & (k == 0)


def sent_left():
    near = 2 * ALONG_Z
    along_x = SIDE * (2 * near + near) + 3 * (16 - near)
    ends = 16 + 3 * (16 - near)
    return rectangle(along_x), (rectangle(ends), rectangle(5 * ends))


def rectangle(tiles):
    return next(
        (tiles // width, width) for width in range(16, 0, -1)
        if tiles % width == 0 and tiles // width <= 2 * SIDE * SIDE
    )


def multiply_part(slab, x, lo, hi, before, target, written=None):
    rows = SIDE * slab.shape[1]
    here = pl.ds(lo, hi - lo)
    left = slab[pl.ds(x * SIDE, SIDE), :, here]
    left = left.reshape(rows, left.shape[2])
    there = pl.ds(pl.multiple_of(x * rows, rows), rows)
    for g in range(SIDE):
        right = slab[SIDE * SIDE + g * SIDE : SIDE * SIDE + (g + 1) * SIDE, :, here]
        product = lax.dot_general(
            left, right.reshape(rows, right.shape[2]), (((1,), (1,)), ((), ())),
            preferred_element_type=jnp.float32,
        )
        columns = slice(g * rows, (g + 1) * rows)
        if before is not None:
            product = product + before[there, columns]
        target[there, columns] = product
        if written is not None:
            written(there, columns, g)


def multiply(slab, partial, out_hbm, out_ref, done):
    n = SIDE
    x = lax.axis_index("col") // n
    copies = []
    for i, dx in enumerate(AHEAD + (2,)):

        def written(there, columns, g, i=i):
            copy = pltpu.make_async_copy(
                out_ref.at[there, columns], out_hbm.at[there, columns], done.at[i * n + g]
            )
            copy.start()
            copies.append(copy)

        ahead = dx in AHEAD
        multiply_part(
            slab, (x + dx) % n, slab.shape[2] // 2 if ahead else 0, slab.shape[2],
            partial if ahead else None, out_ref, written,
        )
    for copy in copies:
        copy.wait()


def on_device(series, lengths, starts):
    rows_dev, steps = series.shape
    blocks = SIDE * SIDE
    vmem = pl.BlockSpec(memory_space=pltpu.VMEM)
    columns = columns_of(steps)
    slots = 2 * blocks + 1
    in_hbm = [
        pltpu.with_memory_space_constraint(array, pltpu.HBM)
        for array in (series, lengths.reshape(1, rows_dev), starts.reshape(1, rows_dev))
    ]
    rows = blocks * rows_dev
    slab, partial = pl.pallas_call(
        functools.partial(kernel, columns, steps),
        out_shape=(
            jax.ShapeDtypeStruct((slots, rows_dev, steps), jnp.bfloat16),
            jax.ShapeDtypeStruct((rows, rows), jnp.float32),
        ),
        in_specs=[pl.BlockSpec(memory_space=pltpu.HBM)] * 3,
        out_specs=(vmem, vmem),
        scratch_shapes=[
            pltpu.VMEM((rows_dev, steps), jnp.float32),
            pltpu.VMEM((1, rows_dev), jnp.int32),
            pltpu.VMEM((1, rows_dev), jnp.int32),
            pltpu.SemaphoreType.DMA((blocks * 4 + (blocks + 1) * 2,)),
            pltpu.SemaphoreType.DMA((3,)),
            pltpu.SemaphoreType.DMA((3,)),
        ],
        compiler_params=pltpu.CompilerParams(
            collective_id=0, has_side_effects=True, vmem_limit_bytes=LIMIT * 2**20
        ),
    )(*in_hbm)
    return pl.pallas_call(
        multiply,
        out_shape=jax.ShapeDtypeStruct((rows, rows), jnp.float32),
        in_specs=[vmem] * 2,
        out_specs=pl.BlockSpec(memory_space=pltpu.HBM),
        scratch_shapes=[
            pltpu.VMEM((rows, rows), jnp.float32),
            pltpu.SemaphoreType.DMA((blocks,)),
        ],
        compiler_params=pltpu.CompilerParams(vmem_limit_bytes=LIMIT * 2**20),
    )(slab, partial)


def solution(mesh):
    in_specs = (P(("row", "col"), None), P(("row", "col")), P(("row", "col")))
    out_specs = P("row", "col")
    return jax.shard_map(
        on_device, mesh=mesh, in_specs=in_specs, out_specs=out_specs, check_vma=False,
    )
```

```python
import functools

import jax
import jax.numpy as jnp
from jax import lax
from jax.experimental import pallas as pl
from jax.experimental.pallas import tpu as pltpu
from jax.sharding import PartitionSpec as P

LANES = 128
SIDE = 4
ALONG_Z = 7
LIMIT = 32
AHEAD = (0, 3, 1)
MESH = pl.DeviceIdType.MESH
ORDER = (
    3, 117, 0, 59, 118, 58, 5, 15, 116, 16, 17, 161, 2, 160, 60, 20, 1, 19, 34, 171, 71,
    18, 120, 187, 12, 186, 4, 119, 142, 208, 14, 13, 224, 36, 22, 144, 21, 45, 209, 114, 9,
    11, 159, 113, 115, 212, 172, 201, 10, 8, 7, 210, 32, 226, 123, 121, 232, 100, 23, 111,
    189, 124, 26, 216, 174, 228, 25, 110, 99, 122, 72, 57, 86, 218, 126, 38, 203, 39, 30,
    98, 102, 140, 175, 108, 162, 74, 109, 83, 40, 185, 101, 28, 44, 61, 225, 184, 41, 234,
    69, 173, 146, 176, 56, 76, 68, 220, 51, 153, 96, 50, 213, 163, 104, 27, 94, 88, 148,
    181, 214, 205, 127, 230, 62, 112, 217, 130, 152, 138, 136, 128, 6, 199, 131, 170, 202,
    63, 222, 164, 90, 135, 143, 75, 35, 178, 158, 196, 188, 84, 73, 236, 89, 93, 182, 238,
    179, 29, 85, 65, 192, 48, 194, 183, 78, 229, 151, 42, 91, 165, 227, 167, 97, 177, 133,
    204, 231, 54, 92, 70, 37, 168, 207, 52, 190, 215, 125, 46, 206, 219, 156, 33, 64, 137,
    95, 132, 67, 166, 47, 211, 43, 235, 103, 195, 239, 157, 197, 105, 55, 147, 193, 66, 87,
    139, 77, 31, 145, 233, 134, 82, 191, 154, 198, 155, 53, 180, 200, 150, 223, 237, 24,
    221, 129, 107, 49, 169, 79, 141, 81, 149, 80, 106,
)


def column_of(row_values):
    n = row_values.shape[1]
    here = lax.broadcasted_iota(jnp.int32, (n, n), 0)
    there = lax.broadcasted_iota(jnp.int32, (n, n), 1)
    picked = jnp.where(here == there, jnp.broadcast_to(row_values, (n, n)), 0)
    return jnp.sum(picked, axis=1, keepdims=True)


def normalize(series, lengths, starts):
    positions = lax.broadcasted_iota(jnp.int32, series.shape, 1)
    inside = (positions >= starts) & (positions < starts + lengths)
    valid_count = lengths.astype(jnp.float32)
    average = jnp.sum(jnp.where(inside, series, 0.0), axis=1, keepdims=True) / valid_count
    centered = jnp.where(inside, series - average, 0.0)
    variance = jnp.sum(centered * centered, axis=1, keepdims=True) / valid_count
    return (centered / jnp.sqrt(valid_count * (variance + 1e-06))).astype(jnp.bfloat16)


def pick(condition, a, b):
    if isinstance(condition, (bool, int)):
        return a if condition else b
    return jnp.where(condition, a, b)


def columns_of(steps):
    half, along = steps // 2, ALONG_Z * LANES
    return [
        (0, along), (along, half), (half, half + along), (half + along, steps),
        (0, half), (half, steps),
    ]


def events_of(r, c):
    n = SIDE
    zh, y, k = r // (2 * n), r // 2 % n, r % 2
    x, z = c // n, c % n

    def row_at(zh, y, k):
        return zh * (2 * n) + y % n * 2 + k

    def col_at(x, z):
        return x % n * n + z

    def c_y(row):
        return row // 2 % n

    events = []
    go = {
        "x+": (True, r, col_at(x + 1, z)),
        "x-": (True, r, col_at(x + n - 1, z)),
        "z+": (z < n - 1, r, c + 1),
        "z-": (z > 0, r, c - 1),
    }

    for half in (4, 5):
        sends = [(z != 0, c, 2 * n * n, half, row_at(zh, y + z, k), c)]
        events.append((("own", half), True, None, sends, []))

    panel = row_at(zh, y + n - z, k)
    home_x, home_z = panel // n, panel % n
    core = (home_x + x) % 2
    here = (home_x == x) & (home_z == z) & (k == 0)
    for half in (4, 5):
        for kind in ("moved", "stays"):
            source = 2 * n * n if kind == "moved" else c
            slot = n * n + c
            sends = [
                (True, source, slot, half, row_at((zh + 1) % 2, y, core),
                 col_at(home_x, home_z)),
                (pick(here, 0, 1) == 1, source, slot, half, row_at(zh, y, core),
                 col_at(home_x, home_z)),
                (here, source, slot, half, None, None),
            ]
            for row in (row_at(zh, y + 1, k), row_at(zh, y + n - 1, k), row_at(zh, y, 1 - k)):
                sends.append((here, slot, slot, half, row, c))
            valid, wait = (z != 0, (2 * n * n, half)) if kind == "moved" else (z == 0, None)
            events.append(((kind, half), valid, wait, sends, []))

    for piece in range(4):
        first, second = piece % 2 == 0, piece // 2
        for dx in (0, 3, 1, 2):
            for dz in range(1 - n, n):
                slot = col_at(x + dx, 0) + z + dz
                valid = (z + dz >= 0) & (z + dz < n)
                def ways(*names):
                    return [
                        (go[way][0], slot, slot, piece, go[way][1], go[way][2])
                        for way in names
                    ]

                def add(kind, sends):
                    events.append(
                        ((kind, dx, dz, piece), valid, None, sends, [(slot, piece)])
                    )

                z_ways = (["z+"] if dz <= 0 else []) + (["z-"] if dz >= 0 else [])
                wait = None if dx == 0 and dz == 0 else (slot, piece)
                urgent = ways(*z_ways) if dx == 0 else []
                events.append((("left", dx, dz, piece), valid, wait, urgent, []))
                if first or dz == 0:
                    if dx == 0:
                        add("near", ways("x+" if second == 0 else "x-"))
                        add("side", ways("x-" if second == 0 else "x+"))
                    elif dx == 3 and second == 0:
                        add("far", ways("x+"))
                    elif dx == 1 and second == 1:
                        add("far", ways("x-"))
                if not first and dx != 0:
                    add("over", ways(*z_ways))

    for j in range(2):
        for dy in (0, 3, 1, 2):
            for half in (4, 5):
                from_z = (y + dy - c_y(c) + n) % n
                slot = n * n + (x + k + 2 * j) % n * n + from_z
                up = (True, slot, slot, half, row_at(zh, y + 1, k), c)
                down = (True, slot, slot, half, row_at(zh, y + n - 1, k), c)
                across = (True, slot, slot, half, row_at(zh, y, 1 - k), c)
                sends = []
                if dy == 0:
                    sends = [up, down] if half == 4 else [down, up]
                elif dy == 3 and half == 4:
                    sends = [up]
                elif dy == 1 and half == 5:
                    sends = [down]
                valid = True
                if dy == 0 and j == 0:
                    valid = pick((k == 0) & (panel == c), 0, 1) == 1
                events.append(
                    (("right", j, dy, half), valid, (slot, half), sends + [across], [])
                )
                slot = n * n + (x + 1 - k + 2 * j) % n * n + from_z
                events.append((("across", j, dy, half), True, (slot, half), [], []))
    if ORDER:
        events = [events[i] for i in ORDER]
    events = [e for e in events if e[3]] + [e for e in events if not e[3]]
    waited = set()
    for i, (name, valid, wait, sends, needs) in enumerate(events):
        if name[0] in ("left", "near", "side", "far", "over"):
            own = name[1] == 0 and name[2] == 0
            first = not own and name[1:] not in waited
            waited.add(name[1:])
            arrival = needs[0] if needs else wait
            events[i] = (name, valid, arrival if first else None, sends, needs)
    return events


def peers_of(r, c):
    n = SIDE
    zh, y, k = r // (2 * n), r // 2 % n, r % 2
    x, z = c // n, c % n
    around = [(True, r, (c + n) % (n * n)), (True, r, (c + 3 * n) % (n * n))]
    around += [(z < n - 1, r, c + 1), (z > 0, r, c - 1)]
    for dy in (1, n - 1):
        around.append((True, zh * 2 * n + (y + dy) % n * 2 + k, c))
    around.append((True, r + 1 - 2 * k, c))
    into, out = list(around), list(around)

    def row_at(zh, y, k):
        return zh * (2 * n) + y % n * 2 + k

    out.append((z != 0, row_at(zh, y + z, k), c))
    into.append((z != 0, row_at(zh, y + n - z, k), c))
    panel = row_at(zh, y + n - z, k)
    for group in range(2):
        row, col = row_at(group, y, (panel // n + x) % 2), panel
        out.append(((row != r) | (col != c), row, col))
        from_z = (y + n - c // 2 % n) % n
        row = row_at(c // (2 * n), y, c % 2)
        col = (x + k + 2 * group) % n * n + from_z
        into.append(((row != r) | (col != c), row, col))
    return into, out


def kernel(
    columns, steps, series_hbm, lengths_hbm, starts_hbm, slab, partial,
    series_ref, lengths_ref, starts_ref, recv, send, load,
):
    r = lax.axis_index("row")
    c = lax.axis_index("col")
    n = SIDE

    loads = [
        pltpu.make_async_copy(source, target, load.at[i])
        for i, (source, target) in enumerate((
            (lengths_hbm, lengths_ref), (starts_hbm, starts_ref), (series_hbm, series_ref),
        ))
    ]
    for copy in loads:
        copy.start()
    into, out = peers_of(r, c)
    barrier = pltpu.get_barrier_semaphore()
    for condition, row, col in into:

        @pl.when(condition)
        def _(row=row, col=col):
            pl.semaphore_signal(
                barrier, inc=1, device_id={"row": row, "col": col}, device_id_type=MESH
            )

    for copy in loads:
        copy.wait()
    slab[c] = normalize(
        series_ref[...], column_of(lengths_ref[...]), column_of(starts_ref[...])
    )
    expected = sum(jnp.where(condition, 1, 0) for condition, _, _ in out)
    pl.semaphore_wait(barrier, expected)

    def arrival_of(slot, piece):
        if piece < 4:
            return slot * 4 + piece
        return n * n * 4 + (slot - n * n) * 2 + piece - 4

    def part(slot, piece):
        lo, hi = columns[piece]
        return slab.at[slot, :, pl.ds(lo, hi - lo)]

    def copy_of(index, source, target, piece, row, col):
        return pltpu.make_async_remote_copy(
            src_ref=part(source, piece),
            dst_ref=part(target, piece),
            send_sem=send.at[index],
            recv_sem=recv.at[arrival_of(target, piece)],
            device_id={"row": row, "col": col},
            device_id_type=MESH,
        )

    def guarded(condition, do):
        if condition is True:
            do()
        else:
            pl.when(condition)(do)

    def handle(group, wait, sends):
        if wait is not None:

            def receive():
                copy_of(group, wait[0], wait[0], wait[1], r, c).wait_recv()

            receive()
        for condition, source, target, piece, row, col in sends:
            if row is None:

                def keep(source=source, target=target, piece=piece):
                    part(target, piece)[...] = part(source, piece)[...]

                guarded(condition, keep)
                continue
            copy = functools.partial(copy_of, group, source, target, piece, row, col)
            guarded(condition, lambda copy=copy: copy().start())

    groups = {"near": 0, "side": 0, "far": 0, "left": 1, "over": 1}
    events = events_of(r, c)
    for name, condition, wait, sends, _ in events:
        if sends:
            group = groups.get(name[0], 2)
            guarded(condition, functools.partial(handle, group, wait, sends))

    def arrive(kind, second, dx=None):
        for name, condition, wait, sends, _ in events:
            if sends or name[0] != kind or wait is None:
                continue
            if kind == "across" and name[3] - 4 != second:
                continue
            if kind == "left" and (name[1] != dx or name[3] // 2 != second):
                continue
            guarded(condition, functools.partial(handle, 2, wait, ()))

    arrive("across", 0)
    for dx in AHEAD:
        arrive("left", 0, dx)
        multiply_part(slab, (c // n + dx) % n, 0, steps // 2, None, partial)
    arrive("left", 0, 2)
    for dx in AHEAD + (2,):
        arrive("left", 1, dx)
    arrive("across", 1)

    def sent(group, blocks, tiles):
        here = slab.at[pl.ds(0, blocks), :, pl.ds(0, tiles * LANES)]
        pltpu.make_async_remote_copy(
            src_ref=here, dst_ref=here, send_sem=send.at[group], recv_sem=recv.at[0],
            device_id={"row": r, "col": c}, device_id_type=MESH,
        ).wait_send()

    x_tiles, z_tiles = sent_left()
    sent(0, *x_tiles)
    z = c % n
    middle = (z > 0) & (z < n - 1)
    guarded(middle, lambda: sent(1, *z_tiles[1]))
    guarded(jnp.logical_not(middle), lambda: sent(1, *z_tiles[0]))
    rights = 15 + jnp.where(z == 0, 0, 1) + jnp.where(stays_here(r, c), 0, 1)
    for blocks in (15, 16, 17):
        guarded(rights == blocks, lambda blocks=blocks: sent(2, blocks, steps // LANES))


def stays_here(r, c):
    n = SIDE
    y, k = r // 2 % n, r % 2
    return (r // (2 * n) * 2 * n + (y + n - c % n) % n * 2 + k == c) & (k == 0)


def sent_left():
    near = 2 * ALONG_Z
    along_x = SIDE * (2 * near + near) + 3 * (16 - near)
    ends = 16 + 3 * (16 - near)
    return rectangle(along_x), (rectangle(ends), rectangle(5 * ends))


def rectangle(tiles):
    return next(
        (tiles // width, width) for width in range(16, 0, -1)
        if tiles % width == 0 and tiles // width <= 2 * SIDE * SIDE
    )


def multiply_part(slab, x, lo, hi, before, target, written=None):
    rows = SIDE * slab.shape[1]
    here = pl.ds(lo, hi - lo)
    left = slab[pl.ds(x * SIDE, SIDE), :, here]
    left = left.reshape(rows, left.shape[2])
    there = pl.ds(pl.multiple_of(x * rows, rows), rows)
    for g in range(SIDE):
        right = slab[SIDE * SIDE + g * SIDE : SIDE * SIDE + (g + 1) * SIDE, :, here]
        product = lax.dot_general(
            left, right.reshape(rows, right.shape[2]), (((1,), (1,)), ((), ())),
            preferred_element_type=jnp.float32,
        )
        columns = slice(g * rows, (g + 1) * rows)
        if before is not None:
            product = product + before[there, columns]
        target[there, columns] = product
        if written is not None:
            written(there, columns, g)


def multiply(slab, partial, out_hbm, out_ref, done):
    n = SIDE
    x = lax.axis_index("col") // n
    copies = []
    for i, dx in enumerate(AHEAD + (2,)):

        def written(there, columns, g, i=i):
            copy = pltpu.make_async_copy(
                out_ref.at[there, columns], out_hbm.at[there, columns], done.at[i * n + g]
            )
            copy.start()
            copies.append(copy)

        ahead = dx in AHEAD
        multiply_part(
            slab, (x + dx) % n, slab.shape[2] // 2 if ahead else 0, slab.shape[2],
            partial if ahead else None, out_ref, written,
        )
    for copy in copies:
        copy.wait()


def on_device(series, lengths, starts):
    rows_dev, steps = series.shape
    blocks = SIDE * SIDE
    vmem = pl.BlockSpec(memory_space=pltpu.VMEM)
    columns = columns_of(steps)
    slots = 2 * blocks + 1
    in_hbm = [
        pltpu.with_memory_space_constraint(array, pltpu.HBM)
        for array in (series, lengths.reshape(1, rows_dev), starts.reshape(1, rows_dev))
    ]
    rows = blocks * rows_dev
    slab, partial = pl.pallas_call(
        functools.partial(kernel, columns, steps),
        out_shape=(
            jax.ShapeDtypeStruct((slots, rows_dev, steps), jnp.bfloat16),
            jax.ShapeDtypeStruct((rows, rows), jnp.float32),
        ),
        in_specs=[pl.BlockSpec(memory_space=pltpu.HBM)] * 3,
        out_specs=(vmem, vmem),
        scratch_shapes=[
            pltpu.VMEM((rows_dev, steps), jnp.float32),
            pltpu.VMEM((1, rows_dev), jnp.int32),
            pltpu.VMEM((1, rows_dev), jnp.int32),
            pltpu.SemaphoreType.DMA((blocks * 4 + (blocks + 1) * 2,)),
            pltpu.SemaphoreType.DMA((3,)),
            pltpu.SemaphoreType.DMA((3,)),
        ],
        compiler_params=pltpu.CompilerParams(
            collective_id=0, has_side_effects=True, vmem_limit_bytes=LIMIT * 2**20
        ),
    )(*in_hbm)
    return pl.pallas_call(
        multiply,
        out_shape=jax.ShapeDtypeStruct((rows, rows), jnp.float32),
        in_specs=[vmem] * 2,
        out_specs=pl.BlockSpec(memory_space=pltpu.HBM),
        scratch_shapes=[
            pltpu.VMEM((rows, rows), jnp.float32),
            pltpu.SemaphoreType.DMA((blocks,)),
        ],
        compiler_params=pltpu.CompilerParams(vmem_limit_bytes=LIMIT * 2**20),
    )(slab, partial)


def solution(mesh):
    in_specs = (P(("row", "col"), None), P(("row", "col")), P(("row", "col")))
    out_specs = P("row", "col")
    return jax.shard_map(
        on_device, mesh=mesh, in_specs=in_specs, out_specs=out_specs, check_vma=False,
    )
```

```python
import functools

import jax
import jax.numpy as jnp
from jax import lax
from jax.experimental import pallas as pl
from jax.experimental.pallas import tpu as pltpu
from jax.sharding import PartitionSpec as P

LANES = 128
SIDE = 4
ALONG_Z = 7
LIMIT = 32
AHEAD = (0, 1, 3)
MESH = pl.DeviceIdType.MESH
ORDER = (
    3, 117, 0, 59, 118, 58, 5, 15, 116, 16, 17, 161, 2, 160, 60, 20, 1, 19, 34, 171, 71,
    18, 120, 187, 12, 186, 4, 119, 142, 208, 14, 13, 224, 36, 22, 144, 21, 45, 209, 114, 9,
    11, 159, 113, 115, 212, 172, 201, 10, 8, 7, 210, 32, 226, 123, 121, 232, 100, 23, 111,
    189, 124, 26, 216, 174, 228, 25, 110, 99, 122, 72, 57, 86, 218, 126, 38, 203, 39, 30,
    98, 102, 140, 175, 108, 162, 74, 109, 83, 40, 185, 101, 28, 44, 61, 225, 184, 41, 234,
    69, 173, 146, 176, 56, 76, 68, 220, 51, 153, 96, 50, 213, 163, 104, 27, 94, 88, 148,
    181, 214, 205, 127, 230, 62, 112, 217, 130, 152, 138, 136, 128, 6, 199, 131, 170, 202,
    63, 222, 164, 90, 135, 143, 75, 35, 178, 158, 196, 188, 84, 73, 236, 89, 93, 182, 238,
    179, 29, 85, 65, 192, 48, 194, 183, 78, 229, 151, 42, 91, 165, 227, 167, 97, 177, 133,
    204, 231, 54, 92, 70, 37, 168, 207, 52, 190, 215, 125, 46, 206, 219, 156, 33, 64, 137,
    95, 132, 67, 166, 47, 211, 43, 235, 103, 195, 239, 157, 197, 105, 55, 147, 193, 66, 87,
    139, 77, 31, 145, 233, 134, 82, 191, 154, 198, 155, 53, 180, 200, 150, 223, 237, 24,
    221, 129, 107, 49, 169, 79, 141, 81, 149, 80, 106,
)


def column_of(row_values):
    n = row_values.shape[1]
    here = lax.broadcasted_iota(jnp.int32, (n, n), 0)
    there = lax.broadcasted_iota(jnp.int32, (n, n), 1)
    picked = jnp.where(here == there, jnp.broadcast_to(row_values, (n, n)), 0)
    return jnp.sum(picked, axis=1, keepdims=True)


def normalize(series, lengths, starts):
    positions = lax.broadcasted_iota(jnp.int32, series.shape, 1)
    inside = (positions >= starts) & (positions < starts + lengths)
    valid_count = lengths.astype(jnp.float32)
    average = jnp.sum(jnp.where(inside, series, 0.0), axis=1, keepdims=True) / valid_count
    centered = jnp.where(inside, series - average, 0.0)
    variance = jnp.sum(centered * centered, axis=1, keepdims=True) / valid_count
    return (centered / jnp.sqrt(valid_count * (variance + 1e-06))).astype(jnp.bfloat16)


def pick(condition, a, b):
    if isinstance(condition, (bool, int)):
        return a if condition else b
    return jnp.where(condition, a, b)


def columns_of(steps):
    half, along = steps // 2, ALONG_Z * LANES
    return [
        (0, along), (along, half), (half, half + along), (half + along, steps),
        (0, half), (half, steps),
    ]


def events_of(r, c):
    n = SIDE
    zh, y, k = r // (2 * n), r // 2 % n, r % 2
    x, z = c // n, c % n

    def row_at(zh, y, k):
        return zh * (2 * n) + y % n * 2 + k

    def col_at(x, z):
        return x % n * n + z

    def c_y(row):
        return row // 2 % n

    events = []
    go = {
        "x+": (True, r, col_at(x + 1, z)),
        "x-": (True, r, col_at(x + n - 1, z)),
        "z+": (z < n - 1, r, c + 1),
        "z-": (z > 0, r, c - 1),
    }

    for half in (4, 5):
        sends = [(z != 0, c, 2 * n * n, half, row_at(zh, y + z, k), c)]
        events.append((("own", half), True, None, sends, []))

    panel = row_at(zh, y + n - z, k)
    home_x, home_z = panel // n, panel % n
    core = (home_x + x) % 2
    here = (home_x == x) & (home_z == z) & (k == 0)
    for half in (4, 5):
        for kind in ("moved", "stays"):
            source = 2 * n * n if kind == "moved" else c
            slot = n * n + c
            sends = [
                (True, source, slot, half, row_at((zh + 1) % 2, y, core),
                 col_at(home_x, home_z)),
                (pick(here, 0, 1) == 1, source, slot, half, row_at(zh, y, core),
                 col_at(home_x, home_z)),
                (here, source, slot, half, None, None),
            ]
            for row in (row_at(zh, y + 1, k), row_at(zh, y + n - 1, k), row_at(zh, y, 1 - k)):
                sends.append((here, slot, slot, half, row, c))
            valid, wait = (z != 0, (2 * n * n, half)) if kind == "moved" else (z == 0, None)
            events.append(((kind, half), valid, wait, sends, []))

    for piece in range(4):
        first, second = piece % 2 == 0, piece // 2
        for dx in (0, 3, 1, 2):
            for dz in range(1 - n, n):
                slot = col_at(x + dx, 0) + z + dz
                valid = (z + dz >= 0) & (z + dz < n)
                def ways(*names):
                    return [
                        (go[way][0], slot, slot, piece, go[way][1], go[way][2])
                        for way in names
                    ]

                def add(kind, sends):
                    events.append(
                        ((kind, dx, dz, piece), valid, None, sends, [(slot, piece)])
                    )

                z_ways = (["z+"] if dz <= 0 else []) + (["z-"] if dz >= 0 else [])
                wait = None if dx == 0 and dz == 0 else (slot, piece)
                urgent = ways(*z_ways) if dx == 0 else []
                events.append((("left", dx, dz, piece), valid, wait, urgent, []))
                if first or dz == 0:
                    if dx == 0:
                        add("near", ways("x+" if second == 0 else "x-"))
                        add("side", ways("x-" if second == 0 else "x+"))
                    elif dx == 3 and second == 0:
                        add("far", ways("x+"))
                    elif dx == 1 and second == 1:
                        add("far", ways("x-"))
                if not first and dx != 0:
                    add("over", ways(*z_ways))

    for j in range(2):
        for dy in (0, 3, 1, 2):
            for half in (4, 5):
                from_z = (y + dy - c_y(c) + n) % n
                slot = n * n + (x + k + 2 * j) % n * n + from_z
                up = (True, slot, slot, half, row_at(zh, y + 1, k), c)
                down = (True, slot, slot, half, row_at(zh, y + n - 1, k), c)
                across = (True, slot, slot, half, row_at(zh, y, 1 - k), c)
                sends = []
                if dy == 0:
                    sends = [up, down] if half == 4 else [down, up]
                elif dy == 3 and half == 4:
                    sends = [up]
                elif dy == 1 and half == 5:
                    sends = [down]
                valid = True
                if dy == 0 and j == 0:
                    valid = pick((k == 0) & (panel == c), 0, 1) == 1
                events.append(
                    (("right", j, dy, half), valid, (slot, half), sends + [across], [])
                )
                slot = n * n + (x + 1 - k + 2 * j) % n * n + from_z
                events.append((("across", j, dy, half), True, (slot, half), [], []))
    if ORDER:
        events = [events[i] for i in ORDER]
    events = [e for e in events if e[3]] + [e for e in events if not e[3]]
    waited = set()
    for i, (name, valid, wait, sends, needs) in enumerate(events):
        if name[0] in ("left", "near", "side", "far", "over"):
            own = name[1] == 0 and name[2] == 0
            first = not own and name[1:] not in waited
            waited.add(name[1:])
            arrival = needs[0] if needs else wait
            events[i] = (name, valid, arrival if first else None, sends, needs)
    return events


def peers_of(r, c):
    n = SIDE
    zh, y, k = r // (2 * n), r // 2 % n, r % 2
    x, z = c // n, c % n
    around = [(True, r, (c + n) % (n * n)), (True, r, (c + 3 * n) % (n * n))]
    around += [(z < n - 1, r, c + 1), (z > 0, r, c - 1)]
    for dy in (1, n - 1):
        around.append((True, zh * 2 * n + (y + dy) % n * 2 + k, c))
    around.append((True, r + 1 - 2 * k, c))
    into, out = list(around), list(around)

    def row_at(zh, y, k):
        return zh * (2 * n) + y % n * 2 + k

    out.append((z != 0, row_at(zh, y + z, k), c))
    into.append((z != 0, row_at(zh, y + n - z, k), c))
    panel = row_at(zh, y + n - z, k)
    for group in range(2):
        row, col = row_at(group, y, (panel // n + x) % 2), panel
        out.append(((row != r) | (col != c), row, col))
        from_z = (y + n - c // 2 % n) % n
        row = row_at(c // (2 * n), y, c % 2)
        col = (x + k + 2 * group) % n * n + from_z
        into.append(((row != r) | (col != c), row, col))
    return into, out


def kernel(
    columns, steps, series_hbm, lengths_hbm, starts_hbm, slab, partial,
    series_ref, lengths_ref, starts_ref, recv, send, load,
):
    r = lax.axis_index("row")
    c = lax.axis_index("col")
    n = SIDE

    loads = [
        pltpu.make_async_copy(source, target, load.at[i])
        for i, (source, target) in enumerate((
            (lengths_hbm, lengths_ref), (starts_hbm, starts_ref), (series_hbm, series_ref),
        ))
    ]
    for copy in loads:
        copy.start()
    into, out = peers_of(r, c)
    barrier = pltpu.get_barrier_semaphore()
    for condition, row, col in into:

        @pl.when(condition)
        def _(row=row, col=col):
            pl.semaphore_signal(
                barrier, inc=1, device_id={"row": row, "col": col}, device_id_type=MESH
            )

    for copy in loads:
        copy.wait()
    slab[c] = normalize(
        series_ref[...], column_of(lengths_ref[...]), column_of(starts_ref[...])
    )
    expected = sum(jnp.where(condition, 1, 0) for condition, _, _ in out)
    pl.semaphore_wait(barrier, expected)

    def arrival_of(slot, piece):
        if piece < 4:
            return slot * 4 + piece
        return n * n * 4 + (slot - n * n) * 2 + piece - 4

    def part(slot, piece):
        lo, hi = columns[piece]
        return slab.at[slot, :, pl.ds(lo, hi - lo)]

    def copy_of(index, source, target, piece, row, col):
        return pltpu.make_async_remote_copy(
            src_ref=part(source, piece),
            dst_ref=part(target, piece),
            send_sem=send.at[index],
            recv_sem=recv.at[arrival_of(target, piece)],
            device_id={"row": row, "col": col},
            device_id_type=MESH,
        )

    def guarded(condition, do):
        if condition is True:
            do()
        else:
            pl.when(condition)(do)

    def handle(group, wait, sends):
        if wait is not None:

            def receive():
                copy_of(group, wait[0], wait[0], wait[1], r, c).wait_recv()

            receive()
        for condition, source, target, piece, row, col in sends:
            if row is None:

                def keep(source=source, target=target, piece=piece):
                    part(target, piece)[...] = part(source, piece)[...]

                guarded(condition, keep)
                continue
            copy = functools.partial(copy_of, group, source, target, piece, row, col)
            guarded(condition, lambda copy=copy: copy().start())

    groups = {"near": 0, "side": 0, "far": 0, "left": 1, "over": 1}
    events = events_of(r, c)
    for name, condition, wait, sends, _ in events:
        if sends:
            group = groups.get(name[0], 2)
            guarded(condition, functools.partial(handle, group, wait, sends))

    def arrive(kind, second, dx=None):
        for name, condition, wait, sends, _ in events:
            if sends or name[0] != kind or wait is None:
                continue
            if kind == "across" and name[3] - 4 != second:
                continue
            if kind == "left" and (name[1] != dx or name[3] // 2 != second):
                continue
            guarded(condition, functools.partial(handle, 2, wait, ()))

    arrive("across", 0)
    for dx in AHEAD:
        arrive("left", 0, dx)
        multiply_part(slab, (c // n + dx) % n, 0, steps // 2, None, partial)
    arrive("left", 0, 2)
    for dx in AHEAD + (2,):
        arrive("left", 1, dx)
    arrive("across", 1)

    def sent(group, blocks, tiles):
        here = slab.at[pl.ds(0, blocks), :, pl.ds(0, tiles * LANES)]
        pltpu.make_async_remote_copy(
            src_ref=here, dst_ref=here, send_sem=send.at[group], recv_sem=recv.at[0],
            device_id={"row": r, "col": c}, device_id_type=MESH,
        ).wait_send()

    x_tiles, z_tiles = sent_left()
    sent(0, *x_tiles)
    z = c % n
    middle = (z > 0) & (z < n - 1)
    guarded(middle, lambda: sent(1, *z_tiles[1]))
    guarded(jnp.logical_not(middle), lambda: sent(1, *z_tiles[0]))
    rights = 15 + jnp.where(z == 0, 0, 1) + jnp.where(stays_here(r, c), 0, 1)
    for blocks in (15, 16, 17):
        guarded(rights == blocks, lambda blocks=blocks: sent(2, blocks, steps // LANES))


def stays_here(r, c):
    n = SIDE
    y, k = r // 2 % n, r % 2
    return (r // (2 * n) * 2 * n + (y + n - c % n) % n * 2 + k == c) & (k == 0)


def sent_left():
    near = 2 * ALONG_Z
    along_x = SIDE * (2 * near + near) + 3 * (16 - near)
    ends = 16 + 3 * (16 - near)
    return rectangle(along_x), (rectangle(ends), rectangle(5 * ends))


def rectangle(tiles):
    return next(
        (tiles // width, width) for width in range(16, 0, -1)
        if tiles % width == 0 and tiles // width <= 2 * SIDE * SIDE
    )


def multiply_part(slab, x, lo, hi, before, target, written=None):
    rows = SIDE * slab.shape[1]
    here = pl.ds(lo, hi - lo)
    left = slab[pl.ds(x * SIDE, SIDE), :, here]
    left = left.reshape(rows, left.shape[2])
    there = pl.ds(pl.multiple_of(x * rows, rows), rows)
    for g in range(SIDE):
        right = slab[SIDE * SIDE + g * SIDE : SIDE * SIDE + (g + 1) * SIDE, :, here]
        product = lax.dot_general(
            left, right.reshape(rows, right.shape[2]), (((1,), (1,)), ((), ())),
            preferred_element_type=jnp.float32,
        )
        columns = slice(g * rows, (g + 1) * rows)
        if before is not None:
            product = product + before[there, columns]
        target[there, columns] = product
        if written is not None:
            written(there, columns, g)


def multiply(slab, partial, out_hbm, out_ref, done):
    n = SIDE
    x = lax.axis_index("col") // n
    copies = []
    for i, dx in enumerate(AHEAD + (2,)):

        def written(there, columns, g, i=i):
            copy = pltpu.make_async_copy(
                out_ref.at[there, columns], out_hbm.at[there, columns], done.at[i * n + g]
            )
            copy.start()
            copies.append(copy)

        ahead = dx in AHEAD
        multiply_part(
            slab, (x + dx) % n, slab.shape[2] // 2 if ahead else 0, slab.shape[2],
            partial if ahead else None, out_ref, written,
        )
    for copy in copies:
        copy.wait()


def on_device(series, lengths, starts):
    rows_dev, steps = series.shape
    blocks = SIDE * SIDE
    vmem = pl.BlockSpec(memory_space=pltpu.VMEM)
    columns = columns_of(steps)
    slots = 2 * blocks + 1
    in_hbm = [
        pltpu.with_memory_space_constraint(array, pltpu.HBM)
        for array in (series, lengths.reshape(1, rows_dev), starts.reshape(1, rows_dev))
    ]
    rows = blocks * rows_dev
    slab, partial = pl.pallas_call(
        functools.partial(kernel, columns, steps),
        out_shape=(
            jax.ShapeDtypeStruct((slots, rows_dev, steps), jnp.bfloat16),
            jax.ShapeDtypeStruct((rows, rows), jnp.float32),
        ),
        in_specs=[pl.BlockSpec(memory_space=pltpu.HBM)] * 3,
        out_specs=(vmem, vmem),
        scratch_shapes=[
            pltpu.VMEM((rows_dev, steps), jnp.float32),
            pltpu.VMEM((1, rows_dev), jnp.int32),
            pltpu.VMEM((1, rows_dev), jnp.int32),
            pltpu.SemaphoreType.DMA((blocks * 4 + (blocks + 1) * 2,)),
            pltpu.SemaphoreType.DMA((3,)),
            pltpu.SemaphoreType.DMA((3,)),
        ],
        compiler_params=pltpu.CompilerParams(
            collective_id=0, has_side_effects=True, vmem_limit_bytes=LIMIT * 2**20
        ),
    )(*in_hbm)
    return pl.pallas_call(
        multiply,
        out_shape=jax.ShapeDtypeStruct((rows, rows), jnp.float32),
        in_specs=[vmem] * 2,
        out_specs=pl.BlockSpec(memory_space=pltpu.HBM),
        scratch_shapes=[
            pltpu.VMEM((rows, rows), jnp.float32),
            pltpu.SemaphoreType.DMA((blocks,)),
        ],
        compiler_params=pltpu.CompilerParams(vmem_limit_bytes=LIMIT * 2**20),
    )(slab, partial)


def solution(mesh):
    in_specs = (P(("row", "col"), None), P(("row", "col")), P(("row", "col")))
    out_specs = P("row", "col")
    return jax.shard_map(
        on_device, mesh=mesh, in_specs=in_specs, out_specs=out_specs, check_vma=False,
    )
```
